32 devices in a mesh: seq: 8 (over y, x, core), head: 4 (over z).
Axes of the slice: x: 2, y: 2, z: 4, core: 2. Of those that a mesh axis runs over, the one named last changes fastest.
Arguments:
- text_states: bfloat16 [2048, 4096], P('seq', 'head'), may hold values from -200 to 200
- query_weight: bfloat16 [4096, 4096], P(None, 'head'), may hold values from -0.09375 to 0.09375
- image_keys: bfloat16 [4096, 1024], P('seq', 'head'), may hold values from -12 to 12
- image_values: bfloat16 [4096, 1024], P('seq', 'head'), may hold values from -24 to 24
- output_weight: bfloat16 [4096, 4096], P('head'), may hold values from -0.09375 to 0.09375
- attn_gate: float32 [1], replicated, may hold values from 0.3 to 1.5
- frame_lengths: int32 [16], replicated, may hold values from 1 to 512, 4096 in all
- frame_limit: int32 [32], replicated, may hold values from 0 to 16
Outputs:
- gated_branch: bfloat16 [2048, 4096], P('seq', 'head')
The draws below stay inside these ranges and needn't reach their ends.
Inputs may be any that keep to these rules, and one draw needn't show every extreme that they name: `frame_lengths`: the lengths sum to 4096.
All inputs are finite; a program needn't handle non-finite values.
Results may differ from the reference program's by a relative error of at most 0.014.
The reference program's roundings to bfloat16 on the way count: a program that leaves them out, or rounds other values in their place, can miss the bound.
Values may be sent and summed in bfloat16 or wider, within the bound.
No kernel may reach another device: no remote copies, remote signals or barrier semaphores. Data moves between devices by JAX's collectives and lax.ppermute only.
A program may use at most 128 MiB of HBM per device.

```python
import math
import jax
import jax.numpy as jnp
import numpy as np
from jax import lax

D = 4096
HEADS = 32
KV_HEADS = 8
HD = 128
VID_DEV = 512
TBLK = 64
GROUP = 4
TEXT = 2048
VIDEO = 4096
FRAMES = 16
TEXT_BLOCKS = 32


def draw_text_states(key, part):
    normal_draw = jax.random.normal(jax.random.fold_in(key, 11), (TEXT, D), jnp.float32)
    return jnp.clip(normal_draw, -200.0, 200.0).astype(jnp.bfloat16)


def touch_ends(drawn, stream_key, low, largest):
    spot = [jax.random.randint(jax.random.fold_in(stream_key, axis), (), 0, length) for axis, length in enumerate(drawn.shape)]
    widest = drawn.shape.index(max(drawn.shape))
    beside = spot[:widest] + [(spot[widest] + 1) % drawn.shape[widest]] + spot[widest + 1:]
    return drawn.at[tuple(spot)].set(low).at[tuple(beside)].set(largest)


def block_scale(stream_key, extent, split, smallest, largest):
    def one(position, blocks):
        heights = jax.random.uniform(jax.random.fold_in(jax.random.fold_in(stream_key, 6), position), (blocks,), jnp.float32, smallest / len(split), largest / len(split))
        return jnp.repeat(jnp.exp(heights), extent[position] // blocks).reshape((-1,) + (1,) * (len(extent) - position - 1))

    factor_of = one(*split[0])
    for cut in split[1:]:
        factor_of = factor_of * one(*cut)
    return factor_of


def length_profile(count, total, reach, lean):
    loads = [(1 << 20) // math.isqrt(standing ** lean) + 1 for standing in range(2, count + 1)]
    rest, given = total - reach - (count - 1), [1] * (count - 1)
    while rest > 0:
        free = [i for i in range(count - 1) if given[i] < reach]
        whole, remaining = sum([loads[i] for i in free]), rest
        for i in free:
            addition = min(reach - given[i], max(1, remaining * loads[i] // whole), rest)
            given[i] = given[i] + addition
            rest = rest - addition
    return np.array([reach] + given)


def uneven(rng, count, total, limit, slope):
    if count == 2:
        one = jax.random.randint(rng, (), max(1, total - limit), min(limit, total - 1) + 1)
        return jnp.stack([one, total - one])
    sizes = jnp.asarray(length_profile(count, total, limit, slope), jnp.int32)
    couples = (count - 1) // 2
    giver, sink = sizes[1:1 + 2 * couples:2], sizes[2:2 + 2 * couples:2]
    margin = jnp.minimum(giver - 1, limit - sink)
    moved = jax.random.randint(jax.random.fold_in(rng, 1), (couples,), 0, 1 << 20) % (margin + 1)
    sizes = sizes.at[1:1 + 2 * couples:2].set(giver - moved).at[2:2 + 2 * couples:2].set(sink + moved)
    return sizes[jax.random.permutation(jax.random.fold_in(rng, 2), count)]


def centred(stream_key, extent, scale, reach, cuts=(), held_as=jnp.bfloat16):
    factor_of = block_scale(stream_key, extent, cuts, -0.22, 0.18) if cuts else 1.0
    drawn = jax.random.normal(stream_key, extent, jnp.float32) * scale * factor_of
    return jnp.minimum(jnp.maximum(drawn, -reach), reach).astype(held_as)


def setup_inputs(seed: int = 0) -> dict:
    keys = jax.random.split(jax.random.key(seed), 9)
    return {
        "text_states": draw_text_states(jax.random.fold_in(keys[8], 71), 0),
        "query_weight": centred(keys[1], (D, HEADS * HD), D ** -0.5, 0.09375, ((1, 4),)),
        "image_keys": centred(keys[2], (VIDEO, KV_HEADS * HD), 2.0, 12.0, ((0, 8), (1, 4))),
        "image_values": centred(keys[3], (VIDEO, KV_HEADS * HD), 4.0, 24.0, ((0, 8), (1, 4))),
        "output_weight": centred(keys[4], (HEADS * HD, D), (HEADS * HD) ** -0.5, 0.09375, ((0, 4),)),
        "attn_gate": jnp.clip(jax.random.uniform(keys[5], (1,), jnp.float32, 0.3, 1.5), 0.3, 1.5),
        "frame_lengths": uneven(keys[6], FRAMES, VIDEO, VID_DEV, 2).astype(jnp.int32),
        "frame_limit": touch_ends(jax.random.randint(keys[7], (TEXT_BLOCKS,), 0, FRAMES + 1), jax.random.fold_in(keys[7], 1), 0, FRAMES).astype(jnp.int32),
    }


masked_fill = -1e+30

def reference(text_states, query_weight, image_keys, image_values, output_weight, attn_gate, frame_lengths, frame_limit):
    queries = jnp.dot(text_states, query_weight, preferred_element_type=jnp.float32).astype(jnp.bfloat16)
    frame_ends = jnp.cumsum(frame_lengths).astype(jnp.int32)
    token_positions = jnp.arange(VIDEO, dtype=jnp.int32)
    key_frames = lax.optimization_barrier(jnp.sum((frame_ends[None, :] <= token_positions[:, None]).astype(jnp.int32), axis=1))
    row_limits = jnp.repeat(frame_limit, TBLK)
    query_heads = queries.reshape(TEXT, HEADS, HD).transpose(1, 0, 2)
    key_head_count = image_keys.reshape(VIDEO, KV_HEADS, HD).transpose(1, 0, 2)
    value_heads = image_values.reshape(VIDEO, KV_HEADS, HD).transpose(1, 0, 2)
    score_scale = 1.0 / math.sqrt(HD)
    block_rows = TEXT // 4

    def one_block(head_no, block_no):
        head_rows = lax.dynamic_index_in_dim(query_heads, head_no, 0, keepdims=False)
        query_rows = lax.dynamic_slice_in_dim(head_rows, block_no * block_rows, block_rows, 0)
        key_rows = lax.dynamic_index_in_dim(key_head_count, head_no // GROUP, 0, keepdims=False)
        value_rows = lax.dynamic_index_in_dim(value_heads, head_no // GROUP, 0, keepdims=False)
        limits = lax.dynamic_slice_in_dim(row_limits, block_no * block_rows, block_rows, 0)
        scores = jnp.dot(query_rows, key_rows.T, preferred_element_type=jnp.float32) * score_scale
        visible = key_frames[None, :] < limits[:, None]
        best_score = lax.optimization_barrier(jnp.max(jnp.where(visible, scores, masked_fill), axis=1))
        weights = jnp.where(visible, jnp.exp(scores - best_score[:, None]), 0.0)
        weight_sum = lax.optimization_barrier(jnp.sum(weights, axis=1))
        mixed = jnp.dot(weights.astype(jnp.bfloat16), value_rows, preferred_element_type=jnp.float32)
        return (mixed / jnp.maximum(weight_sum, 1.0)[:, None]).astype(jnp.bfloat16)

    def one_head(head_no):
        blocks = lax.map(lambda block_no: one_block(head_no, block_no), jnp.arange(4, dtype=jnp.int32))
        return blocks.reshape(TEXT, HD)
    heads_out = lax.map(one_head, jnp.arange(HEADS, dtype=jnp.int32))
    attention_output = heads_out.transpose(1, 0, 2).reshape(TEXT, HEADS * HD)
    projected = jnp.dot(attention_output, output_weight, preferred_element_type=jnp.float32)
    return (jnp.tanh(attn_gate[0]) * projected).astype(jnp.bfloat16)
```

```python
import functools
import math

import jax
import jax.numpy as jnp
from jax import lax
from jax.experimental import pallas as pl
from jax.experimental.pallas import tpu as pltpu
from jax.sharding import PartitionSpec as P

HD = 128
TBLK = 64
GROUP = 4
CHUNKS = 2
KEY_TILE = 512


masked_fill = -1e30

VMEM = pl.BlockSpec(memory_space=pltpu.VMEM)
SMEM = pl.BlockSpec(memory_space=pltpu.SMEM)


def swap(block, axis, bit):
    route = [(i, i ^ bit) for i in range(lax.axis_size(axis))]
    return lax.ppermute(block, axis, route)


def xor_gather(block, bits):
    stacks = [(block[None], [0])]
    for bit in bits:
        if bit != bits[-1] and len(stacks) > 1:
            merged = jnp.concatenate([stack for stack, _ in stacks], axis=0)
            stacks = [(merged, [o for _, offsets in stacks for o in offsets])]
        stacks = stacks + [
            (swap(stack, "seq", 1 << bit), [o ^ (1 << bit) for o in offsets])
            for stack, offsets in stacks
        ]
    return stacks


def assemble_kernel(key_offsets, value_offsets, *refs):
    key_parts = refs[: len(key_offsets)]
    value_parts = refs[len(key_offsets) : -2]
    keys_out, values_out = refs[-2:]
    me = lax.axis_index("seq")
    for part, offsets in zip(key_parts, key_offsets):
        rows = part.shape[1]
        for j, offset in enumerate(offsets):
            start = pl.multiple_of(jnp.bitwise_xor(me, offset) * rows, rows)
            keys_out[pl.ds(start, rows), :] = part[j]
    for part, offsets in zip(value_parts, value_offsets):
        rows = part.shape[2]
        for j, offset in enumerate(offsets):
            start = pl.multiple_of(jnp.bitwise_xor(me, offset) * rows, rows)
            values_out[:, pl.ds(start, rows)] = part[j]


def chunk_kernel(
    first_block,
    device_blocks,
    lengths_ref,
    limits_ref,
    own_ref,
    near_ref,
    far_ref,
    middle_ref,
    forward_ref,
    query_weight_ref,
    keys_ref,
    values_ref,
    output_weight_ref,
    across_out,
    far_out,
    near_out,
    own_out,
    text_scr,
    query_scr,
    attention_scr,
    mixed_scr,
):
    rows, part = own_ref.shape
    blocks = rows // TBLK
    head_index = lax.axis_index("head")
    last_head = lax.axis_size("head") - 1
    local_kv = query_scr.shape[1]
    score_scale = math.log2(math.e) / math.sqrt(HD)

    def columns(distance):
        return pl.multiple_of(jnp.bitwise_xor(head_index, distance) * part, part)

    text_scr[:, pl.ds(columns(0), part)] = own_ref[...]
    text_scr[:, pl.ds(columns(1), part)] = near_ref[...]
    text_scr[:, pl.ds(columns(2), part)] = far_ref[...]
    at_end = jnp.logical_or(head_index == 0, head_index == last_head)

    @pl.when(at_end)
    def _():
        text_scr[:, pl.ds(columns(3), part)] = forward_ref[...]

    @pl.when(jnp.logical_not(at_end))
    def _():
        text_scr[:, pl.ds(columns(3), part)] = middle_ref[...]

    width = 2 * HD
    for n in range(query_weight_ref.shape[1] // width):
        product = jnp.dot(
            text_scr[...],
            query_weight_ref[:, n * width : (n + 1) * width],
            preferred_element_type=jnp.float32,
        ).astype(jnp.bfloat16)
        for j in range(2):
            kv, g = divmod(2 * n + j, GROUP)
            for b in range(blocks):
                query_scr[b, kv, g * TBLK : (g + 1) * TBLK, :] = product[
                    b * TBLK : (b + 1) * TBLK, j * HD : (j + 1) * HD
                ]

    lanes = GROUP * TBLK

    def attend_block(b, _):
        limit = limits_ref[lax.axis_index("seq") * device_blocks + first_block + b]
        visible_rows = lax.fori_loop(
            0, limit, lambda f, total: total + lengths_ref[f], jnp.int32(0)
        )
        mixed_scr[...] = jnp.zeros_like(mixed_scr)

        def tile(start, carry, masked):
            out = []
            for kv in range(local_kv):
                best, total = carry[kv]
                scores = lax.dot_general(
                    keys_ref[pl.ds(start, KEY_TILE), kv * HD : (kv + 1) * HD],
                    query_scr[b, kv],
                    (((1,), (1,)), ((), ())),
                    preferred_element_type=jnp.float32,
                )
                if masked:
                    position = start + lax.broadcasted_iota(jnp.int32, scores.shape, 0)
                    scores = jnp.where(position < visible_rows, scores, masked_fill)
                new_best = jnp.maximum(best, jnp.max(scores, axis=0, keepdims=True))
                weights = jnp.exp2((scores - new_best) * score_scale)
                factor = jnp.exp2((best - new_best) * score_scale)
                total = total * factor + jnp.sum(
                    weights.reshape(KEY_TILE // 8, 8, lanes), axis=0
                )
                mixed_scr[kv] = mixed_scr[kv] * factor + jnp.dot(
                    values_ref[kv * HD : (kv + 1) * HD, pl.ds(start, KEY_TILE)],
                    weights.astype(jnp.bfloat16),
                    preferred_element_type=jnp.float32,
                )
                out.append((new_best, total))
            return tuple(out)

        carry = tuple(
            (jnp.full((1, lanes), masked_fill, jnp.float32), jnp.zeros((8, lanes), jnp.float32))
            for _ in range(local_kv)
        )
        full_tiles = visible_rows // KEY_TILE
        carry = lax.fori_loop(
            0,
            full_tiles,
            lambda t, c: tile(pl.multiple_of(t * KEY_TILE, KEY_TILE), c, False),
            carry,
        )
        tail = jnp.where(visible_rows % KEY_TILE > 0, 1, 0)
        carry = lax.fori_loop(
            full_tiles,
            full_tiles + tail,
            lambda t, c: tile(pl.multiple_of(t * KEY_TILE, KEY_TILE), c, True),
            carry,
        )
        for kv in range(local_kv):
            total = jnp.sum(carry[kv][1], axis=0, keepdims=True)
            mixed = (mixed_scr[kv] / jnp.maximum(total, 1.0)).T.astype(jnp.bfloat16)
            for g in range(GROUP):
                head = kv * GROUP + g
                attention_scr[pl.ds(pl.multiple_of(b * TBLK, TBLK), TBLK), head * HD : (head + 1) * HD] = (
                    mixed[g * TBLK : (g + 1) * TBLK]
                )
        return 0

    lax.fori_loop(0, blocks, attend_block, 0)

    for distance, out in ((3, across_out), (2, far_out), (1, near_out), (0, own_out)):
        for n in range(part // width):
            start = pl.multiple_of(columns(distance) + n * width, width)
            out[:, n * width : (n + 1) * width] = jnp.dot(
                attention_scr[...],
                output_weight_ref[:, pl.ds(start, width)],
                preferred_element_type=jnp.float32,
            ).astype(out.dtype)


def shards(
    text_states,
    query_weight,
    image_keys,
    image_values,
    output_weight,
    attn_gate,
    frame_lengths,
    frame_limit,
):
    text_rows, part = text_states.shape
    video_rows, kv_columns = image_keys.shape
    local_kv = kv_columns // HD
    heads_axis = lax.axis_size("head")
    seq_size = lax.axis_size("seq")
    assert heads_axis == 4 and seq_size & (seq_size - 1) == 0
    seq_bits = seq_size.bit_length() - 1
    middle = [(1, 2), (2, 1)]
    to_ends = [(2, 3), (1, 0)]
    from_ends = [(3, 2), (0, 1)]
    device_blocks = text_rows // TBLK
    chunk_rows = text_rows // CHUNKS

    def gather_text(chunk):
        far = swap(chunk, "head", 2)
        near = swap(chunk, "head", 1)
        mid = lax.ppermute(chunk, "head", middle)
        forward = lax.ppermute(far, "head", to_ends)
        return chunk, near, far, mid, forward

    up_bits = list(range(1, seq_bits))
    key_stacks = xor_gather(image_keys, up_bits + [0])
    value_stacks = xor_gather(image_values.T, up_bits[::-1] + [0])
    texts = []
    after = None
    for c in range(CHUNKS):
        chunk = text_states[c * chunk_rows : (c + 1) * chunk_rows]
        if after is not None:
            chunk, _ = lax.optimization_barrier((chunk, after))
        texts.append(gather_text(chunk))
        after = texts[-1][2]

    all_rows = seq_size * video_rows
    keys, values = pl.pallas_call(
        functools.partial(
            assemble_kernel, [o for _, o in key_stacks], [o for _, o in value_stacks]
        ),
        in_specs=[VMEM] * (len(key_stacks) + len(value_stacks)),
        out_specs=[VMEM, VMEM],
        out_shape=[
            jax.ShapeDtypeStruct((all_rows, kv_columns), jnp.bfloat16),
            jax.ShapeDtypeStruct((kv_columns, all_rows), jnp.bfloat16),
        ],
        cost_estimate=pl.CostEstimate(
            flops=1 << 20, bytes_accessed=4 * all_rows * kv_columns * 2, transcendentals=0
        ),
        name="assemble",
    )(*[s for s, _ in key_stacks], *[s for s, _ in value_stacks])

    heads_columns = query_weight.shape[1]
    flops = (
        4 * chunk_rows * query_weight.size
        + 4 * chunk_rows * all_rows * heads_columns
    )
    gated = []
    gate = jnp.tanh(attn_gate[0])
    for c in range(CHUNKS):
        shape = jax.ShapeDtypeStruct((chunk_rows, part), jnp.bfloat16)
        across, far, near, own = pl.pallas_call(
            functools.partial(chunk_kernel, c * (chunk_rows // TBLK), device_blocks),
            in_specs=[SMEM, SMEM] + [VMEM] * 9,
            out_specs=[VMEM] * 4,
            out_shape=[shape] * 3 + [jax.ShapeDtypeStruct((chunk_rows, part), jnp.float32)],
            scratch_shapes=[
                pltpu.VMEM((chunk_rows, heads_axis * part), jnp.bfloat16),
                pltpu.VMEM((chunk_rows // TBLK, local_kv, GROUP * TBLK, HD), jnp.bfloat16),
                pltpu.VMEM((chunk_rows, heads_columns), jnp.bfloat16),
                pltpu.VMEM((local_kv, HD, GROUP * TBLK), jnp.float32),
            ],
            cost_estimate=pl.CostEstimate(
                flops=flops,
                bytes_accessed=2 * (query_weight.size + output_weight.size),
                transcendentals=chunk_rows * all_rows * local_kv * GROUP,
            ),
            name="chunk",
        )(frame_lengths, frame_limit, *texts[c], query_weight, keys, values, output_weight)
        added = lax.ppermute(across, "head", from_ends)
        near_in = swap(near, "head", 1)
        mid_in = lax.ppermute(across, "head", middle)
        far_in = swap(
            (far.astype(jnp.float32) + added.astype(jnp.float32)).astype(jnp.bfloat16), "head", 2
        )
        total = own
        for received in (near_in, mid_in, far_in):
            total = total + received.astype(jnp.float32)
        gated.append((gate * total).astype(jnp.bfloat16))
    return jnp.concatenate(gated, axis=0)


def solution(mesh):
    in_specs = (
        P("seq", "head"),
        P(None, "head"),
        P("seq", "head"),
        P("seq", "head"),
        P("head", None),
        P(),
        P(),
        P(),
    )
    out_specs = P("seq", "head")
    return jax.shard_map(shards, mesh=mesh, in_specs=in_specs, out_specs=out_specs, check_vma=False)
```

```python
import functools
import math

import jax
import jax.numpy as jnp
from jax import lax
from jax.experimental import pallas as pl
from jax.experimental.pallas import tpu as pltpu
from jax.sharding import PartitionSpec as P


HD = 128
TBLK = 64
GROUP = 4
CHUNKS = 2
KEY_TILE = 512


masked_fill = -1e30

VMEM = pl.BlockSpec(memory_space=pltpu.VMEM)
SMEM = pl.BlockSpec(memory_space=pltpu.SMEM)


def swap(block, axis, bit):
    route = [(i, i ^ bit) for i in range(lax.axis_size(axis))]
    return lax.ppermute(block, axis, route)


def xor_gather(block, bits):
    stacks = [(block[None], [0])]
    for bit in bits:
        if bit != bits[-1] and len(stacks) > 1:
            merged = jnp.concatenate([stack for stack, _ in stacks], axis=0)
            stacks = [(merged, [o for _, offsets in stacks for o in offsets])]
        received = []
        for stack, offsets in stacks:
            moved = swap(stack, "seq", 1 << bit)
            received.append((moved, [o ^ (1 << bit) for o in offsets]))
        stacks = stacks + received
    return stacks


def stage_kernel(first_ref, second_ref, first_out, second_out, sems):
    copies = [
        pltpu.make_async_copy(first_ref, first_out, sems.at[0]),
        pltpu.make_async_copy(second_ref, second_out, sems.at[1]),
    ]
    for copy in copies:
        copy.start()
    for copy in copies:
        copy.wait()


def assemble_kernel(key_offsets, value_offsets, *refs):
    key_parts = refs[: len(key_offsets)]
    value_parts = refs[len(key_offsets) : -2]
    keys_out, values_out = refs[-2:]
    me = lax.axis_index("seq")
    for part, offsets in zip(key_parts, key_offsets):
        rows = part.shape[1]
        for j, offset in enumerate(offsets):
            start = pl.multiple_of(jnp.bitwise_xor(me, offset) * rows, rows)
            keys_out[pl.ds(start, rows), :] = part[j]
    for part, offsets in zip(value_parts, value_offsets):
        rows = part.shape[2]
        for j, offset in enumerate(offsets):
            start = pl.multiple_of(jnp.bitwise_xor(me, offset) * rows, rows)
            values_out[:, pl.ds(start, rows)] = part[j]


def chunk_kernel(
    first_block,
    device_blocks,
    lengths_ref,
    limits_ref,
    own_ref,
    near_ref,
    far_ref,
    middle_ref,
    forward_ref,
    query_weight_ref,
    keys_ref,
    values_ref,
    output_weight_ref,
    across_out,
    far_out,
    near_out,
    own_out,
    text_scr,
    query_scr,
    attention_scr,
    mixed_scr,
    *score_refs,
):
    rows, part = own_ref.shape
    blocks = rows // TBLK
    head_index = lax.axis_index("head")
    last_head = lax.axis_size("head") - 1
    local_kv = query_scr.shape[1]
    score_scale = math.log2(math.e) / math.sqrt(HD)

    def columns(distance):
        return pl.multiple_of(jnp.bitwise_xor(head_index, distance) * part, part)

    text_scr[:, pl.ds(columns(0), part)] = own_ref[...]
    text_scr[:, pl.ds(columns(1), part)] = near_ref[...]
    text_scr[:, pl.ds(columns(2), part)] = far_ref[...]
    at_end = jnp.logical_or(head_index == 0, head_index == last_head)

    @pl.when(at_end)
    def _():
        text_scr[:, pl.ds(columns(3), part)] = forward_ref[...]

    @pl.when(jnp.logical_not(at_end))
    def _():
        text_scr[:, pl.ds(columns(3), part)] = middle_ref[...]

    width = 2 * HD
    for n in range(query_weight_ref.shape[1] // width):
        product = jnp.dot(
            text_scr[...],
            query_weight_ref[:, n * width : (n + 1) * width],
            preferred_element_type=jnp.float32,
        ).astype(jnp.bfloat16)
        for j in range(2):
            kv, g = divmod(2 * n + j, GROUP)
            for b in range(blocks):
                query_scr[b, kv, g * TBLK : (g + 1) * TBLK, :] = product[
                    b * TBLK : (b + 1) * TBLK, j * HD : (j + 1) * HD
                ]

    lanes = GROUP * TBLK

    def attend_block(b, _):
        limit = limits_ref[lax.axis_index("seq") * device_blocks + first_block + b]
        visible_rows = lax.fori_loop(
            0, limit, lambda f, total: total + lengths_ref[f], jnp.int32(0)
        )
        mixed_scr[...] = jnp.zeros_like(mixed_scr)

        def score(kv, t):
            start = pl.multiple_of(t * KEY_TILE, KEY_TILE)
            score_refs[kv][...] = lax.dot_general(
                keys_ref[pl.ds(start, KEY_TILE), kv * HD : (kv + 1) * HD],
                query_scr[b, kv],
                (((1,), (1,)), ((), ())),
                preferred_element_type=jnp.float32,
            )

        def consume(kv, t, state, masked):
            best, total = state
            start = pl.multiple_of(t * KEY_TILE, KEY_TILE)
            scores = score_refs[kv][...]
            if masked:
                position = start + lax.broadcasted_iota(jnp.int32, scores.shape, 0)
                scores = jnp.where(position < visible_rows, scores, masked_fill)
            new_best = jnp.maximum(best, jnp.max(scores, axis=0, keepdims=True))
            weights = jnp.exp2((scores - new_best) * score_scale)
            factor = jnp.exp2((best - new_best) * score_scale)
            total = total * factor + jnp.sum(weights.reshape(KEY_TILE // 8, 8, lanes), axis=0)
            mixed_scr[kv] = mixed_scr[kv] * factor + jnp.dot(
                values_ref[kv * HD : (kv + 1) * HD, pl.ds(start, KEY_TILE)],
                weights.astype(jnp.bfloat16),
                preferred_element_type=jnp.float32,
            )
            return new_best, total

        def tile(t, carry, last):
            out = []
            for kv in range(local_kv):
                if kv + 1 < local_kv:
                    score(kv + 1, t)
                elif not last:
                    score(0, t + 1)
                out.append(consume(kv, t, carry[kv], last))
            return tuple(out)

        carry = tuple(
            (jnp.full((1, lanes), masked_fill, jnp.float32), jnp.zeros((8, lanes), jnp.float32))
            for _ in range(local_kv)
        )
        tiles = (visible_rows + KEY_TILE - 1) // KEY_TILE
        last_tile = jnp.maximum(tiles - 1, 0)

        @pl.when(tiles > 0)
        def _():
            score(0, 0)

        carry = lax.fori_loop(0, last_tile, lambda t, c: tile(t, c, False), carry)
        carry = lax.fori_loop(last_tile, tiles, lambda t, c: tile(t, c, True), carry)
        for kv in range(local_kv):
            total = jnp.sum(carry[kv][1], axis=0, keepdims=True)
            mixed = (mixed_scr[kv] / jnp.maximum(total, 1.0)).T.astype(jnp.bfloat16)
            for g in range(GROUP):
                head = kv * GROUP + g
                block_rows = pl.ds(pl.multiple_of(b * TBLK, TBLK), TBLK)
                attention_scr[block_rows, head * HD : (head + 1) * HD] = mixed[
                    g * TBLK : (g + 1) * TBLK
                ]
        return 0

    lax.fori_loop(0, blocks, attend_block, 0)

    for distance, out in ((3, across_out), (2, far_out), (1, near_out), (0, own_out)):
        for n in range(part // width):
            start = pl.multiple_of(columns(distance) + n * width, width)
            out[:, n * width : (n + 1) * width] = jnp.dot(
                attention_scr[...],
                output_weight_ref[:, pl.ds(start, width)],
                preferred_element_type=jnp.float32,
            ).astype(out.dtype)


def shards(
    text_states,
    query_weight,
    image_keys,
    image_values,
    output_weight,
    attn_gate,
    frame_lengths,
    frame_limit,
):
    text_rows, part = text_states.shape
    video_rows, kv_columns = image_keys.shape
    local_kv = kv_columns // HD
    heads_axis = lax.axis_size("head")
    seq_size = lax.axis_size("seq")
    assert heads_axis == 4 and seq_size & (seq_size - 1) == 0
    seq_bits = seq_size.bit_length() - 1
    middle = [(1, 2), (2, 1)]
    to_ends = [(2, 3), (1, 0)]
    from_ends = [(3, 2), (0, 1)]
    device_blocks = text_rows // TBLK
    chunk_rows = text_rows // CHUNKS

    def gather_text(chunk):
        far = swap(chunk, "head", 2)
        near = swap(chunk, "head", 1)
        mid = lax.ppermute(chunk, "head", middle)
        forward = lax.ppermute(far, "head", to_ends)
        return chunk, near, far, mid, forward

    up_bits = list(range(1, seq_bits))
    key_stacks = xor_gather(image_keys, up_bits + [0])
    value_stacks = xor_gather(image_values.T, up_bits[::-1] + [0])
    texts = []
    after = None
    for c in range(CHUNKS):
        rows = text_states
        if after is not None:
            rows, _ = lax.optimization_barrier((rows, after))
        texts.append(gather_text(rows[c * chunk_rows : (c + 1) * chunk_rows]))
        after = texts[-1][2]

    query_weight, output_weight = pl.pallas_call(
        stage_kernel,
        in_specs=[pl.BlockSpec(memory_space=pltpu.HBM)] * 2,
        out_specs=[VMEM] * 2,
        out_shape=[jax.ShapeDtypeStruct(w.shape, w.dtype) for w in (query_weight, output_weight)],
        scratch_shapes=[pltpu.SemaphoreType.DMA((2,))],
        compiler_params=pltpu.CompilerParams(vmem_limit_bytes=4 << 20),
        name="stage",
    )(query_weight, output_weight)

    all_rows = seq_size * video_rows
    keys, values = pl.pallas_call(
        functools.partial(
            assemble_kernel, [o for _, o in key_stacks], [o for _, o in value_stacks]
        ),
        in_specs=[VMEM] * (len(key_stacks) + len(value_stacks)),
        out_specs=[VMEM, VMEM],
        out_shape=[
            jax.ShapeDtypeStruct((all_rows, kv_columns), jnp.bfloat16),
            jax.ShapeDtypeStruct((kv_columns, all_rows), jnp.bfloat16),
        ],
        cost_estimate=pl.CostEstimate(
            flops=1 << 20, bytes_accessed=4 * all_rows * kv_columns * 2, transcendentals=0
        ),
        compiler_params=pltpu.CompilerParams(
            vmem_limit_bytes=2 * 4 * all_rows * kv_columns + (2 << 20)
        ),
        name="assemble",
    )(*[s for s, _ in key_stacks], *[s for s, _ in value_stacks])

    heads_columns = query_weight.shape[1]
    flops = (
        4 * chunk_rows * query_weight.size
        + 4 * chunk_rows * all_rows * heads_columns
    )
    gated = []
    gate = jnp.tanh(attn_gate[0])
    for c in range(CHUNKS):
        shape = jax.ShapeDtypeStruct((chunk_rows, part), jnp.bfloat16)
        across, far, near, own = pl.pallas_call(
            functools.partial(chunk_kernel, c * (chunk_rows // TBLK), device_blocks),
            in_specs=[SMEM, SMEM] + [VMEM] * 9,
            out_specs=[VMEM] * 4,
            out_shape=[shape] * 3 + [jax.ShapeDtypeStruct((chunk_rows, part), jnp.float32)],
            scratch_shapes=[
                pltpu.VMEM((chunk_rows, heads_axis * part), jnp.bfloat16),
                pltpu.VMEM((chunk_rows // TBLK, local_kv, GROUP * TBLK, HD), jnp.bfloat16),
                pltpu.VMEM((chunk_rows, heads_columns), jnp.bfloat16),
                pltpu.VMEM((local_kv, HD, GROUP * TBLK), jnp.float32),
            ]
            + [pltpu.VMEM((KEY_TILE, GROUP * TBLK), jnp.float32)] * local_kv,
            compiler_params=pltpu.CompilerParams(vmem_limit_bytes=12 << 20),
            cost_estimate=pl.CostEstimate(
                flops=flops,
                bytes_accessed=2 * (query_weight.size + output_weight.size),
                transcendentals=chunk_rows * all_rows * local_kv * GROUP,
            ),
            name="chunk",
        )(frame_lengths, frame_limit, *texts[c], query_weight, keys, values, output_weight)
        added = lax.ppermute(across, "head", from_ends)
        near_in = swap(near, "head", 1)
        mid_in = lax.ppermute(across, "head", middle)
        far = (far.astype(jnp.float32) + added.astype(jnp.float32)).astype(jnp.bfloat16)
        far_in = swap(far, "head", 2)
        total = own
        for received in (near_in, mid_in, far_in):
            total = total + received.astype(jnp.float32)
        gated.append((gate * total).astype(jnp.bfloat16))
    return jnp.concatenate(gated, axis=0)


def solution(mesh):
    in_specs = (
        P("seq", "head"),
        P(None, "head"),
        P("seq", "head"),
        P("seq", "head"),
        P("head", None),
        P(),
        P(),
        P(),
    )
    out_specs = P("seq", "head")

    return jax.shard_map(shards, mesh=mesh, in_specs=in_specs, out_specs=out_specs, check_vma=False)
```
